256 devices in a mesh: groups: 2 (over z), expert: 64 (over y, x), tensor: 2 (over core).
Axes of the slice: x: 8, y: 8, z: 2, core: 2. Of those that a mesh axis runs over, the one named last changes fastest.
The devices are a block of a 8x8x16 slice.
Arguments:
- hidden_in: bfloat16 [2048, 3584], P(('groups', 'expert')), parts along dimension 0, may hold values from -6 to 6
- batch_len: int32 [2], P('groups'), parts along dimension 0, may hold values from 256 to 1024
- expert_ids: int32 [2048, 8], P(('groups', 'expert')), parts along dimension 0, may hold values from 0 to 63, all different within a row; in each aligned block of 16 rows (0 to 15, 16 to 31, ...) at most 3 rows name the same one
- gate_num: int32 [2048, 8], P(('groups', 'expert')), parts along dimension 0, may hold values from 1 to 1024
- w_gate: bfloat16 [64, 3584, 1024], P('expert', None, 'tensor'), may hold values from -0.09375 to 0.09375
- w_up: bfloat16 [64, 3584, 1024], P('expert', None, 'tensor'), may hold values from -0.09375 to 0.09375
- w_down: bfloat16 [64, 1024, 3584], P('expert', 'tensor'), may hold values from -0.1875 to 0.1875
- q_latent: bfloat16 [4, 64, 512], P('groups', 'tensor'), parts along dimension 0, may hold values from -117 to 117
- q_rope: bfloat16 [4, 64, 64], P('groups', 'tensor'), parts along dimension 0, may hold values from -6 to 6
- kv_latent: bfloat16 [4, 8192, 512], P('groups', 'expert'), parts along dimension 0, may hold values from -4 to 4
- kv_rope: bfloat16 [4, 64, 8192], P('groups', None, 'expert'), parts along dimension 0, may hold values from -4 to 4
- ctx_len: int32 [4], P('groups'), parts along dimension 0, may hold values from 1 to 8192, as said below
Outputs:
- moe_out: bfloat16 [2048, 3584], P(('groups', 'expert')), parts along dimension 0
- attn_out: bfloat16 [4, 64, 512], P('groups', 'tensor'), parts along dimension 0
The draws below stay inside these ranges and needn't reach their ends.
There are 2 independent parts, one for each index of `groups`. The reference program is written for one: setup_inputs(seed, part) draws one part's arguments, and reference() takes and returns one part's arrays. A program takes and returns all parts, laid end to end along the dimension named above; an argument that names none is the same for every part. Nothing has to cross between parts.
Inputs may be any that keep to these rules, and one draw needn't show every extreme that they name: `expert_ids`: each row names 8 different experts; the 16 rows of one index of the expert axis name any one expert at most 3 times. `batch_len`: the live slots are the first ones of the replica. `ctx_len`: the first request's context fills all 8192 positions.
All inputs are finite; a program needn't handle non-finite values.
Results may differ from the reference program's by a relative error of at most 0.0028.
The reference program's roundings to bfloat16 on the way count: a program that leaves them out, or rounds other values in their place, can miss the bound.
Values may be sent and summed in bfloat16 or wider, within the bound.
A program may use at most 64 MiB of HBM per device.

```python
import math
import jax
import jax.numpy as jnp
import numpy as np
from jax import lax

D = 3584
FF = 1024
TOPK = 8
H = 64
LAT = 512
ROPE = 64
TOK_DEV = 16
BATCH = 2
EXPERTS = 64
TOKENS = 1024
CAP = 3
CTX = 8192
N_EXPERT = 64


def cache_pair(key):
    base = jax.random.fold_in(key, 71)
    first, second = jax.random.split(base)
    latent = jax.random.truncated_normal(first, -4.0, 4.0, (BATCH, CTX, LAT), jnp.float32)
    rotary = jax.random.truncated_normal(second, -4.0, 4.0, (BATCH, ROPE, CTX), jnp.float32)
    return (latent, rotary)


def draw_kv_latent(key, part):
    return cache_pair(key)[0].astype(jnp.bfloat16)


def draw_kv_rope(key, part):
    return cache_pair(key)[1].astype(jnp.bfloat16)


def draw_ctx_len(key, part):
    lengths = jax.random.randint(jax.random.fold_in(key, 53), (BATCH,), 1, CTX + 1, dtype=jnp.int32)
    first = jnp.arange(BATCH, dtype=jnp.int32) == 0
    return jnp.where(first, CTX, lengths).astype(jnp.int32)


def draw_q_latent(key, part):
    noise = jax.random.truncated_normal(jax.random.fold_in(key, 37), -4.0, 4.0, (BATCH, H, LAT), jnp.float32)
    latent = cache_pair(key)[0]
    head_anchor = latent[:, 0, :] + latent[:, 1, :]
    tail_anchor = latent[:, CTX - 2, :] + latent[:, CTX - 1, :]
    first = (jnp.arange(BATCH, dtype=jnp.int32) == 0)[:, None]
    anchor = jnp.where(first, tail_anchor, head_anchor)
    length_sq = jnp.sum(anchor * anchor, axis=1) + 1.0
    heads = jnp.arange(H, dtype=jnp.int32)
    strength = 250.0 + 150.0 * (heads // 2 % 3).astype(jnp.float32)
    chosen = heads % 2 == 0
    direction = anchor * 192.0 ** 0.5 / length_sq[:, None]
    aligned = strength[None, :, None] * direction[:, None, :]
    mixed = jnp.where(chosen[None, :, None], aligned, noise)
    bound = float(60000 // LAT)
    return jnp.clip(mixed, -bound, bound).astype(jnp.bfloat16)


def touch_ends(drawn, own_key, smallest, top_value):
    dims = drawn.shape
    spot = [jax.random.randint(jax.random.fold_in(own_key, axis), (), 0, dims[axis]) for axis in range(len(dims))]
    drawn = drawn.at[tuple(spot)].set(smallest)
    longest = dims.index(max(dims))
    spot[longest] = (spot[longest] + 1) % dims[longest]
    return drawn.at[tuple(spot)].set(top_value)


def block_levels(own_key, extent, pieces, low, largest):
    def one(axis_at, shards_of):
        draws = jax.random.uniform(jax.random.fold_in(jax.random.fold_in(own_key, 6), axis_at), (shards_of,), jnp.float32, low / len(pieces), largest / len(pieces))
        return jnp.repeat(jnp.exp(draws), extent[axis_at] // shards_of).reshape((-1,) + (1,) * (len(extent) - axis_at - 1))

    factor_of = one(*pieces[0])
    for cut in pieces[1:]:
        factor_of = factor_of * one(*cut)
    return factor_of


def assign_block(stream_key, own, number, rows, count, top, reach, slope):
    order = jax.random.permutation(stream_key, count)
    heavy_load, ordinary = shares(count, rows * top, reach, slope, True), shares(count, rows * top, reach, slope, False)
    places = jnp.arange(count)

    def named(sizes, offset_by):
        used = int((sizes > 0).sum())
        fixed = max(1, used // 4)
        shifted = fixed + (places - fixed + offset_by * (used - fixed)) % max(1, count - fixed)
        return jnp.zeros((count,), jnp.int32).at[order[jnp.where(places < fixed, places, shifted)]].set(jnp.asarray(sizes, jnp.int32))

    sizes = jnp.where(number % 4 == 0, named(heavy_load, number // 4), named(ordinary, number - number // 4 - 1))
    mixed = jax.random.permutation(jax.random.fold_in(own, 3), count)
    donor, taker = mixed[0:count // 2 * 2:2], mixed[1:count // 2 * 2:2]
    margin = jnp.minimum(sizes[donor] - 1, reach - sizes[taker]) // 2
    margin = jnp.where((donor == order[0]) | (taker == order[0]) | (sizes[taker] == 0), 0, jnp.maximum(margin, 0))
    shifted = jax.random.randint(jax.random.fold_in(own, 4), (count // 2,), 0, 1 << 20) % (margin + 1)
    sizes = sizes.at[donor].add(-shifted).at[taker].add(shifted)
    items = jnp.searchsorted(jnp.cumsum(sizes), jnp.arange(rows * top), side="right").astype(jnp.int32)
    listing = items.reshape(top, rows).T
    listing = listing[jax.random.permutation(jax.random.fold_in(own, 1), rows)]
    offset_by = jax.random.randint(jax.random.fold_in(own, 2), (rows, 1), 0, top)
    return jnp.take_along_axis(listing, (jnp.arange(top)[None, :] + offset_by) % top, axis=1)


def shares(count, total, most, skew, full):
    loads = [(1 << 20) // math.isqrt(grade ** skew) + 1 for grade in range(1, count + 1)]
    largest = most if full else min(most, max(-(-total // count), total * loads[0] // sum(loads)))
    least = 1 if total - largest >= count - 1 else 0
    holding, rest = [largest] + [least] * (count - 1), total - largest - least * (count - 1)
    while rest > 0:
        free = [i for i in range(1, count) if holding[i] < largest] or [i for i in range(1, count) if holding[i] < most]
        pool, budget = sum([loads[i] for i in free]), rest
        for i in free:
            more = min(most - holding[i], max(1, budget * loads[i] // pool), rest)
            holding[i] = holding[i] + more
            rest = rest - more
    return np.array(holding)


def gaussian(stream_key, shape, width, reach, cuts=(), kind=jnp.bfloat16):
    values = width * jax.random.normal(stream_key, shape, jnp.float32)
    if cuts:
        values = values * block_levels(stream_key, shape, cuts, -0.22, 0.18)
    return jnp.clip(values, -reach, reach).astype(kind)


def setup_inputs(seed: int = 0, part: int = 0) -> dict:
    key_of = jax.random.split(jax.random.key(seed), 13)
    own_keys = jax.random.split(jax.random.fold_in(key_of[12], part), 13)
    hidden_in = gaussian(own_keys[0], (TOKENS, D), 1.0, 6.0, ((0, 64),))
    batch_len = jax.random.randint(own_keys[1], (1,), TOKENS // 4, TOKENS + 1).astype(jnp.int32)
    expert_ids_keys = jax.random.split(jax.random.fold_in(own_keys[2], 1), TOKENS // TOK_DEV)
    expert_ids_turns = jax.random.permutation(jax.random.fold_in(own_keys[2], 3), TOKENS // TOK_DEV)
    expert_ids = jax.vmap(lambda own, number: assign_block(jax.random.fold_in(own_keys[2], 2), own, number, TOK_DEV, EXPERTS, TOPK, CAP, 2))(expert_ids_keys, expert_ids_turns).reshape((TOKENS, TOPK))
    gate_num = touch_ends(jax.random.randint(own_keys[3], (TOKENS, TOPK), 1, 1025), jax.random.fold_in(own_keys[3], 1), 1, 1024).astype(jnp.int32)
    w_gate = gaussian(key_of[4], (EXPERTS, D, FF), D ** -0.5, 0.09375, ((0, 64), (2, 2)))
    w_up = gaussian(key_of[5], (EXPERTS, D, FF), D ** -0.5, 0.09375, ((0, 64), (2, 2)))
    w_down = gaussian(key_of[6], (EXPERTS, FF, D), FF ** -0.5, 0.1875, ((0, 64), (1, 2)))
    q_latent = draw_q_latent(jax.random.fold_in(jax.random.fold_in(key_of[12], part), 71), part)
    q_rope = gaussian(own_keys[8], (BATCH, H, ROPE), 1.0, 6.0, ((1, 2),))
    kv_latent = draw_kv_latent(jax.random.fold_in(jax.random.fold_in(key_of[12], part), 71), part)
    kv_rope = draw_kv_rope(jax.random.fold_in(jax.random.fold_in(key_of[12], part), 71), part)
    ctx_len = draw_ctx_len(jax.random.fold_in(jax.random.fold_in(key_of[12], part), 71), part)
    return dict(hidden_in=hidden_in, batch_len=batch_len, expert_ids=expert_ids, gate_num=gate_num, w_gate=w_gate, w_up=w_up, w_down=w_down, q_latent=q_latent, q_rope=q_rope, kv_latent=kv_latent, kv_rope=kv_rope, ctx_len=ctx_len)


gate_denominator = 1024.0
softmax_scale = 192.0 ** -0.5


def reference(hidden_in, batch_len, expert_ids, gate_num, w_gate, w_up, w_down, q_latent, q_rope, kv_latent, kv_rope, ctx_len):
    live = jnp.arange(TOKENS, dtype=jnp.int32) < batch_len[0]
    flat_expert = expert_ids.reshape(-1)
    token_of = jnp.arange(TOKENS * TOPK, dtype=jnp.int32) // TOPK
    live_pick = live[token_of]
    weight = jnp.where(live_pick, gate_num.reshape(-1).astype(jnp.float32) / gate_denominator, 0.0)
    rows_most = N_EXPERT * CAP

    def one_expert(total, index):
        match = (flat_expert == index) & live_pick
        picked = jnp.nonzero(match, size=rows_most, fill_value=0)[0].astype(jnp.int32)
        valid = jnp.arange(rows_most, dtype=jnp.int32) < jnp.sum(match.astype(jnp.int32))
        tokens = token_of[picked]
        rows = hidden_in[tokens]
        gate = jnp.dot(rows, w_gate[index], preferred_element_type=jnp.float32)
        upper = jnp.dot(rows, w_up[index], preferred_element_type=jnp.float32)
        hidden = (jax.nn.silu(gate) * upper).astype(jnp.bfloat16)
        value = jnp.dot(hidden, w_down[index], preferred_element_type=jnp.float32).astype(jnp.bfloat16)
        value = lax.optimization_barrier(value).astype(jnp.float32)
        scaled = value * jnp.where(valid, weight[picked], 0.0)[:, None]
        return total.at[tokens].add(scaled), None

    start = jnp.zeros((TOKENS, D), jnp.float32)
    summed, unused = lax.scan(one_expert, start, jnp.arange(EXPERTS, dtype=jnp.int32))
    moe_out = summed.astype(jnp.bfloat16)

    scores = jnp.einsum("bhl,bpl->bhp", q_latent.astype(jnp.float32), kv_latent.astype(jnp.float32))
    scores = scores + jnp.einsum("bhr,brp->bhp", q_rope.astype(jnp.float32), kv_rope.astype(jnp.float32))
    scores = scores * softmax_scale
    valid_pos = jnp.arange(CTX, dtype=jnp.int32)[None, :] < ctx_len[:, None]
    scores = jnp.where(valid_pos[:, None, :], scores, -1e30)
    top = jnp.max(scores, axis=2, keepdims=True)
    probs = jnp.where(valid_pos[:, None, :], jnp.exp(scores - top), 0.0)
    total = jnp.sum(probs, axis=2, keepdims=True)
    probs_bf = lax.optimization_barrier(probs.astype(jnp.bfloat16)).astype(jnp.float32)
    weighted = jnp.einsum("bhp,bpl->bhl", probs_bf, kv_latent.astype(jnp.float32))
    attn_out = (weighted / total).astype(jnp.bfloat16)
    return moe_out, attn_out
```

```python
import functools

import jax
import jax.numpy as jnp
from jax import lax
from jax.experimental import pallas as pl
from jax.experimental.pallas import tpu as pltpu
from jax.sharding import Mesh
from jax.sharding import PartitionSpec as P

MESH = pl.DeviceIdType.MESH
EXPERT = ("expert_0", "expert_1")
GROUPS_EXPERT = ("groups", "expert_0", "expert_1")
AXES = ("groups", "expert_0", "expert_1", "tensor")

gate_denominator = 1024.0
softmax_scale = 192.0 ** (-0.5)
SLOTS = 3
F32 = jnp.float32
BF16 = jnp.bfloat16


def split_widths(width, parts):
    unit = 256 if width % 256 == 0 else 128
    units = width // unit
    sizes = [units // parts + (1 if k < units % parts else 0) for k in range(parts)]
    return [s * unit for s in sizes if s]


def dot(a, b):
    return jnp.dot(a, b, preferred_element_type=F32)


def kernel(
    n,
    cd,
    cr,
    batch_ref,
    ctx_ref,
    idst_ref,
    ids_ref,
    gate_ref,
    hid_ref,
    wg_hbm,
    wu_hbm,
    wd_hbm,
    ql_ref,
    qr_ref,
    kl_ref,
    kr_ref,
    moe_ref,
    attn_ref,
    wg,
    wu,
    wdo,
    wdx,
    idr,
    gx,
    pk,
    xo,
    xx,
    px,
    pr,
    vb,
    vr,
    ub,
    ur,
    as0,
    ar0,
    as1,
    ar1,
    as2,
    acc,
    wsem,
    s_id,
    s_g,
    s_x,
    s_d,
    s_p,
    s_v,
    s_u,
    s_a,
    s_o,
):
    log = n.bit_length() - 1
    tok = hid_ref.shape[0]
    topk = ids_ref.shape[1]
    half = hid_ref.shape[1] // 2
    rows = n * n * SLOTS
    blk = n * SLOTS
    g = lax.axis_index("groups")
    y = lax.axis_index("expert_0")
    x = lax.axis_index("expert_1")
    c = lax.axis_index("tensor")
    A = y + c * (x - y)
    B = x + c * (y - x)
    sa = n + c * (1 - n)
    sb = 1 + c * (n - 1)
    order = sorted(range(1, n), key=lambda k: (-min(k, n - k), k))

    def on_a(off):
        p = lax.rem(A + off, n)
        return (g, p + c * (y - p), x + c * (p - x), c)

    def on_b(off):
        p = lax.rem(B + off, n)
        return (g, y + c * (p - y), p + c * (x - p), c)

    partner = (g, y, x, 1 - c)
    sent = []

    def copy(src, dst, sems, device):
        made = pltpu.make_async_remote_copy(
            src_ref=src,
            dst_ref=dst,
            send_sem=sems.at[0],
            recv_sem=sems.at[1],
            device_id=device,
            device_id_type=MESH,
        )
        sent.append(made)
        return made

    barrier = pltpu.get_barrier_semaphore()
    for off in order:
        pl.semaphore_signal(barrier, inc=1, device_id=on_a(off), device_id_type=MESH)
        pl.semaphore_signal(barrier, inc=1, device_id=on_b(off), device_id_type=MESH)
    pl.semaphore_signal(barrier, inc=1, device_id=partner, device_id_type=MESH)

    own = pl.multiple_of(c * half, 128)
    oth = pl.multiple_of((1 - c) * half, 128)
    loads = [
        pltpu.make_async_copy(wg_hbm.at[pl.ds(own, half), :], wg.at[0], wsem.at[0]),
        pltpu.make_async_copy(wu_hbm.at[pl.ds(own, half), :], wu.at[0], wsem.at[1]),
        pltpu.make_async_copy(wg_hbm.at[pl.ds(oth, half), :], wg.at[1], wsem.at[2]),
        pltpu.make_async_copy(wu_hbm.at[pl.ds(oth, half), :], wu.at[1], wsem.at[3]),
        pltpu.make_async_copy(wd_hbm.at[:, pl.ds(oth, half)], wdx, wsem.at[4]),
        pltpu.make_async_copy(wd_hbm.at[:, pl.ds(own, half)], wdo, wsem.at[5]),
    ]
    for load in loads:
        load.start()

    nb, nh, lat = ql_ref.shape
    ctx = kl_ref.shape[1]
    per = nb * nh // n
    first = (y * n + x) * ctx
    for b in range(nb):
        scores = lax.dot_general(
            ql_ref[b], kl_ref[b], (((1,), (1,)), ((), ())), preferred_element_type=F32
        )
        scores = scores + dot(qr_ref[b], kr_ref[b])
        position = first + lax.broadcasted_iota(jnp.int32, scores.shape, 1)
        valid = position < ctx_ref[b]
        scores = jnp.where(valid, scores * softmax_scale, -1e30)
        peak = jnp.max(scores, axis=1, keepdims=True)
        probs = jnp.where(valid, jnp.exp(scores - peak), 0.0)
        total = jnp.sum(probs, axis=1, keepdims=True)
        weighted = dot(probs.astype(BF16), kl_ref[b])
        lane = lax.broadcasted_iota(jnp.int32, (nh, 128), 1)
        stats = jnp.where(lane < 64, peak, total)
        for k in range(nh // per):
            as0[b * (nh // per) + k, :, :lat] = weighted[k * per : (k + 1) * per]
            as0[b * (nh // per) + k, :, lat:] = stats[k * per : (k + 1) * per]

    def joined(parts):
        peaks = [p[:, lat : lat + 1] for p in parts]
        totals = [p[:, lat + 64 : lat + 65] for p in parts]
        top = functools.reduce(jnp.maximum, peaks)
        scales = [jnp.exp(p - top) for p in peaks]
        total = sum(t * s for t, s in zip(totals, scales))
        weighted = sum(p[:, :lat] * s for p, s in zip(parts, scales))
        return top, total, weighted

    for q, (at, w) in enumerate(cd):
        gx[q][0] = hid_ref[:, pl.ds(pl.multiple_of(own + at, 128), w)]

    pl.semaphore_wait(barrier, 2 * (n - 1) + 1)

    id_copies = [copy(idst_ref, idr.at[off], s_id.at[:, off], on_a(off)) for off in order]
    for made in id_copies:
        made.start()
    g_copies = []
    for q, (at, w) in enumerate(cd):
        source = hid_ref.at[:, pl.ds(pl.multiple_of(own + at, 128), w)]
        g_copies.append(
            [copy(source, gx[q].at[off], s_g.at[:, q, off], on_a(off)) for off in order]
        )
        for made in g_copies[-1]:
            made.start()
    a0 = []
    for off in order:
        block = lax.rem(A + off, n)
        a0.append(copy(as0.at[block], ar0.at[off], s_a.at[:, 0, off], on_a(off)))
        a0[-1].start()

    r_col = lax.broadcasted_iota(jnp.int32, (rows, 1), 0)

    def parts_of(r):
        q = lax.shift_right_logical(r * 171, 9)
        return lax.shift_right_logical(q, log), q & (n - 1), r - q * SLOTS

    first_of, second_of, slot_of = parts_of(r_col)
    for made in id_copies:
        made.wait_recv()
    lines = n * tok
    lane_t = lax.broadcasted_iota(jnp.int32, (topk, lines), 1)
    line_ids = idst_ref[...]
    for off in range(1, n):
        line_ids = jnp.where(lane_t // tok == off, idr[off], line_ids)
    lane_1 = lax.broadcasted_iota(jnp.int32, (1, lines), 1)
    back = lane_1 // tok
    owner = sa * ((A - back + n) & (n - 1)) + sb * B
    live = owner * tok + (lane_1 & (tok - 1)) < batch_ref[0]
    wanted = sa * A + sb * ((B + first_of) & (n - 1))
    match = line_ids[0:1, :] == wanted
    for k in range(1, topk):
        match = match | (line_ids[k : k + 1, :] == wanted)
    match = match & live & (back == second_of)
    match = match.astype(F32)
    t_row = lax.broadcasted_iota(jnp.int32, (lines, lines), 0)
    t_col = lax.broadcasted_iota(jnp.int32, (lines, lines), 1)
    before = jnp.where(t_row < t_col, 1.0, 0.0).astype(BF16)
    rank = dot(match.astype(BF16), before)
    pick = jnp.where(rank == slot_of.astype(F32), match, 0.0).astype(BF16)

    swap_to = ((second_of << log) + first_of) * SLOTS + slot_of
    swap = jnp.where(lax.broadcasted_iota(jnp.int32, (rows, rows), 1) == swap_to, 1.0, 0.0).astype(
        BF16
    )

    x_copies = []
    for q, (at, w) in enumerate(cd):
        for made in g_copies[q]:
            made.wait_recv()
        packed = dot(pick, gx[q][...].reshape(lines, w))
        xo[q][0] = packed[:blk].astype(BF16)
        for off in range(1, n):
            pk[q][off] = packed[off * blk : (off + 1) * blk].astype(BF16)
        x_copies.append(
            [copy(pk[q].at[off], xo[q].at[off], s_x.at[:, q, off], on_b(off)) for off in order]
        )
        for made in x_copies[-1]:
            made.start()

    for made in a0:
        made.wait_recv()
    top, total, weighted = joined([as0[A]] + [ar0[off] for off in range(1, n)])
    lane = lax.broadcasted_iota(jnp.int32, (per, 128), 1)
    as1[:, :lat] = weighted
    as1[:, lat:] = jnp.where(lane < 64, top, total)
    a1 = [copy(as1, ar1.at[off], s_a.at[:, 1, off], on_b(off)) for off in order]
    for made in a1:
        made.start()

    ff = wg.shape[2]
    for load in loads[:4]:
        load.wait()
    for q, (at, w) in enumerate(cd):
        d_copies = [copy(xo[q].at[0], xx[q].at[0], s_d.at[:, q, 0], partner)]
        d_copies[0].start()
        for k, off in enumerate(reversed(order)):
            x_copies[q][len(order) - 1 - k].wait_recv()
            d_copies.append(copy(xo[q].at[off], xx[q].at[off], s_d.at[:, q, off], partner))
            d_copies[-1].start()
        mine = xo[q][...].reshape(rows, w)
        gate = dot(mine, wg[0, at : at + w, :])
        upper = dot(mine, wu[0, at : at + w, :])
        if q:
            gate = gate + acc[:, :ff]
            upper = upper + acc[:, ff:]
        for made in d_copies:
            made.wait_recv()
        other = dot(swap, xx[q][...].reshape(rows, w)).astype(BF16)
        gate = gate + dot(other, wg[1, at : at + w, :])
        upper = upper + dot(other, wu[1, at : at + w, :])
        if q < len(cd) - 1:
            acc[:, :ff] = gate
            acc[:, ff:] = upper
    hidden = (gate / (1.0 + jnp.exp(-gate)) * upper).astype(BF16)
    turned = dot(swap, hidden).astype(BF16)

    loads[4].wait()
    loads[5].wait()
    p_copies = []
    for q, (at, w) in enumerate(cr):
        px[q][...] = dot(turned, wdx[:, at : at + w])
        p_copies.append(copy(px[q], pr[q], s_p.at[:, q], partner))
        p_copies[-1].start()
    v_copies = []
    for q, (at, w) in enumerate(cr):
        value = dot(hidden, wdo[:, at : at + w])
        p_copies[q].wait_recv()
        value = value + pr[q][...]
        vr[q][0] = value[:blk].astype(BF16)
        for off in range(1, n):
            vb[q][off] = value[off * blk : (off + 1) * blk].astype(BF16)
        v_copies.append(
            [copy(vb[q].at[off], vr[q].at[off], s_v.at[:, q, off], on_b(n - off)) for off in order]
        )
        for made in v_copies[-1]:
            made.start()

    for made in a1:
        made.wait_recv()
    top, total, weighted = joined([as1[...]] + [ar1[off] for off in range(1, n)])
    as2[A] = (weighted / total).astype(BF16)
    a2 = [copy(as2.at[A], as2.at[A], s_a.at[:, 2, off], on_a(off)) for off in order]
    for made in a2:
        made.start()

    r_lane = lax.broadcasted_iota(jnp.int32, (1, rows), 1)
    first_l, second_l, slot_l = parts_of(r_lane)
    named = sa * ((A + first_l) & (n - 1)) + sb * ((B + second_l) & (n - 1))
    ids = ids_ref[...]
    gates = gate_ref[...].astype(F32) / gate_denominator
    here = jnp.zeros((tok, rows), F32)
    weight = jnp.zeros((tok, rows), F32)
    for k in range(topk):
        same = ids[:, k : k + 1] == named
        here = jnp.where(same, 1.0, here)
        weight = jnp.where(same, gates[:, k : k + 1], weight)
    token = (sa * A + sb * B) * tok + lax.broadcasted_iota(jnp.int32, (tok, 1), 0)
    token_live = token < batch_ref[0]
    here = jnp.where(token_live, here, 0.0)
    r_tok = lax.broadcasted_iota(jnp.int32, (tok, tok), 0)
    c_tok = lax.broadcasted_iota(jnp.int32, (tok, tok), 1)
    earlier = jnp.where(c_tok < r_tok, 1.0, 0.0).astype(BF16)
    rank = dot(earlier, here.astype(BF16))
    weight = jnp.where((rank == slot_l.astype(F32)) & (here > 0.0), weight, 0.0)
    high = weight.astype(BF16)
    low = (weight - high.astype(F32)).astype(BF16)

    u_copies = []
    for q, (at, w) in enumerate(cr):
        for made in v_copies[q]:
            made.wait_recv()
        back_rows = dot(swap, vr[q][...].reshape(rows, w))
        ur[q][0] = back_rows[:blk].astype(BF16)
        for off in range(1, n):
            ub[q][off] = back_rows[off * blk : (off + 1) * blk].astype(BF16)
        u_copies.append(
            [copy(ub[q].at[off], ur[q].at[off], s_u.at[:, q, off], on_a(n - off)) for off in order]
        )
        for made in u_copies[-1]:
            made.start()

    for made in a2:
        made.wait_recv()
    attn_ref[...] = as2[...].reshape(nb, nh, lat)

    o_copies = []
    for q, (at, w) in enumerate(cr):
        for made in u_copies[q]:
            made.wait_recv()
        arrived = ur[q][...].reshape(rows, w)
        here_at = pl.ds(pl.multiple_of(own + at, 128), w)
        moe_ref[:, here_at] = (dot(high, arrived) + dot(low, arrived)).astype(BF16)
        o_copies.append(
            copy(moe_ref.at[:, here_at], moe_ref.at[:, here_at], s_o.at[:, q], partner)
        )
        o_copies[-1].start()
    for made in o_copies:
        made.wait_recv()
    for made in sent:
        made.wait_send()


def starts(widths):
    at, found = 0, []
    for w in widths:
        found.append((at, w))
        at += w
    return found


def local(
    hidden_in,
    batch_len,
    expert_ids,
    gate_num,
    w_gate,
    w_up,
    w_down,
    q_latent,
    q_rope,
    kv_latent,
    kv_rope,
    ctx_len,
):
    n = lax.axis_size("expert_0")
    tok, width = hidden_in.shape
    half = width // 2
    ff = w_gate.shape[2]
    nb, nh, lat = q_latent.shape
    per = nb * nh // n
    blk = n * SLOTS
    rows = n * blk
    cd = starts(split_widths(half, 2))
    cr = starts(split_widths(half, 2))
    ids_t = jnp.tile(expert_ids.T, (1, n))
    vmem = pl.BlockSpec(memory_space=pltpu.VMEM)
    smem = pl.BlockSpec(memory_space=pltpu.SMEM)
    hbm = pl.BlockSpec(memory_space=pl.ANY)
    V = pltpu.VMEM
    dma = pltpu.SemaphoreType.DMA
    qd, qr = len(cd), len(cr)
    scratch = [
        V((2, half, ff), BF16),
        V((2, half, ff), BF16),
        V((ff, half), BF16),
        V((ff, half), BF16),
        V((n, *ids_t.shape), jnp.int32),
        [V((n, tok, w), BF16) for _, w in cd],
        [V((n, blk, w), BF16) for _, w in cd],
        [V((n, blk, w), BF16) for _, w in cd],
        [V((n, blk, w), BF16) for _, w in cd],
        [V((rows, w), F32) for _, w in cr],
        [V((rows, w), F32) for _, w in cr],
        [V((n, blk, w), BF16) for _, w in cr],
        [V((n, blk, w), BF16) for _, w in cr],
        [V((n, blk, w), BF16) for _, w in cr],
        [V((n, blk, w), BF16) for _, w in cr],
        V((n, per, lat + 128), F32),
        V((n, per, lat + 128), F32),
        V((per, lat + 128), F32),
        V((n, per, lat + 128), F32),
        V((n, per, lat), BF16),
        V((rows, 2 * ff), F32),
        dma((6,)),
        dma((2, n)),
        dma((2, qd, n)),
        dma((2, qd, n)),
        dma((2, qd, n)),
        dma((2, qr)),
        dma((2, qr, n)),
        dma((2, qr, n)),
        dma((2, 3, n)),
        dma((2, qr)),
    ]
    return pl.pallas_call(
        functools.partial(kernel, n, cd, cr),
        out_shape=(
            jax.ShapeDtypeStruct((tok, width), BF16),
            jax.ShapeDtypeStruct((nb, nh, lat), BF16),
        ),
        in_specs=[smem, smem, vmem, vmem, vmem, vmem, hbm, hbm, hbm, vmem, vmem, vmem, vmem],
        out_specs=(vmem, vmem),
        scratch_shapes=scratch,
        compiler_params=pltpu.CompilerParams(
            collective_id=0, has_side_effects=True, vmem_limit_bytes=56 * 1024 * 1024
        ),
        name="layer_step",
    )(
        batch_len,
        ctx_len,
        ids_t,
        expert_ids,
        gate_num,
        hidden_in,
        w_gate[0],
        w_up[0],
        w_down[0],
        q_latent,
        q_rope,
        kv_latent,
        kv_rope,
    )


def solution(mesh):
    owners = mesh.shape["expert"]
    side = 1
    while side * side < owners:
        side *= 2
    finer = Mesh(
        mesh.devices.reshape(mesh.shape["groups"], side, owners // side, mesh.shape["tensor"]),
        AXES,
    )
    in_specs = (
        P(GROUPS_EXPERT, None),
        P("groups"),
        P(GROUPS_EXPERT, None),
        P(GROUPS_EXPERT, None),
        P(EXPERT, None, "tensor"),
        P(EXPERT, None, "tensor"),
        P(EXPERT, "tensor", None),
        P("groups", "tensor", None),
        P("groups", "tensor", None),
        P("groups", EXPERT, None),
        P("groups", None, EXPERT),
        P("groups"),
    )
    out_specs = (P(GROUPS_EXPERT, None), P("groups", "tensor", None))
    return jax.shard_map(local, mesh=finer, in_specs=in_specs, out_specs=out_specs, check_vma=False)
```

```python
import functools

import jax
import jax.numpy as jnp
from jax import lax
from jax.experimental import pallas as pl
from jax.experimental.pallas import tpu as pltpu
from jax.sharding import Mesh
from jax.sharding import PartitionSpec as P

MESH = pl.DeviceIdType.MESH
EXPERT = ("expert_0", "expert_1")
GROUPS_EXPERT = ("groups", "expert_0", "expert_1")
AXES = ("groups", "expert_0", "expert_1", "tensor")

gate_denominator = 1024.0
softmax_scale = 192.0 ** (-0.5)
SLOTS = 3
KEEP = True
ND = 3
NR = 3
F32 = jnp.float32
BF16 = jnp.bfloat16


def split_widths(width, parts):
    unit = 256 if width % 256 == 0 else 128
    units = width // unit
    sizes = [units // parts + (1 if k < units % parts else 0) for k in range(parts)]
    return [s * unit for s in sizes if s]


def dot(a, b):
    return jnp.dot(a, b, preferred_element_type=F32)


def kernel(
    n,
    cd,
    cr,
    batch_ref,
    ctx_hbm,
    ids_hbm,
    gate_hbm,
    hid_hbm,
    wg_hbm,
    wu_hbm,
    wd_hbm,
    ql_hbm,
    qr_hbm,
    kl_hbm,
    kr_hbm,
    moe_ref,
    attn_ref,
    ctx_ref,
    ids_ref,
    gate_ref,
    ql_ref,
    qr_ref,
    kl_ref,
    kr_ref,
    wg,
    wu,
    wdo,
    wdr,
    ids0,
    idr,
    gx,
    pk,
    xo,
    xx,
    hs,
    hr,
    va,
    vb,
    vr,
    ub,
    ur,
    as0,
    ar0,
    as1,
    ar1,
    as2,
    acc,
    lsem,
    s_w,
    s_id,
    s_g,
    s_x,
    s_d,
    s_h,
    s_v,
    s_u,
    s_a,
    s_o,
):
    log = n.bit_length() - 1
    topk, tok = ids_ref.shape
    ff = wg.shape[2]
    half = hid_hbm.shape[1] // 2
    rows = n * n * SLOTS
    blk = n * SLOTS
    lines = n * tok
    g = lax.axis_index("groups")
    y = lax.axis_index("expert_0")
    x = lax.axis_index("expert_1")
    c = lax.axis_index("tensor")
    A = y + c * (x - y)
    B = x + c * (y - x)
    sa = n + c * (1 - n)
    sb = 1 + c * (n - 1)
    order = sorted(range(1, n), key=lambda k: (-min(k, n - k), k))
    own = pl.multiple_of(c * half, 128)
    oth = pl.multiple_of((1 - c) * half, 128)

    def on_a(off):
        p = lax.rem(A + off, n)
        return (g, p + c * (y - p), x + c * (p - x), c)

    def on_b(off):
        p = lax.rem(B + off, n)
        return (g, y + c * (p - y), p + c * (x - p), c)

    partner = (g, y, x, 1 - c)
    sent = []

    def copy(src, dst, sems, device):
        made = pltpu.make_async_remote_copy(
            src_ref=src,
            dst_ref=dst,
            send_sem=sems.at[0],
            recv_sem=sems.at[1],
            device_id=device,
            device_id_type=MESH,
        )
        sent.append(made)
        return made

    def arrive(name, copies):
        with jax.named_scope(name):
            for made in copies:
                made.wait_recv()

    barrier = pltpu.get_barrier_semaphore()
    for off in order:
        pl.semaphore_signal(barrier, inc=1, device_id=on_a(off), device_id_type=MESH)
        pl.semaphore_signal(barrier, inc=1, device_id=on_b(off), device_id_type=MESH)
    pl.semaphore_signal(barrier, inc=1, device_id=partner, device_id_type=MESH)

    started = []

    def load(src, dst):
        made = pltpu.make_async_copy(src, dst, lsem.at[len(started)])
        made.start()
        started.append(made)
        return made

    hid_loads = []
    for q, (at, w) in enumerate(cd):
        here_at = pl.ds(pl.multiple_of(own + at, 128), w)
        hid_loads.append(load(hid_hbm.at[:, here_at], gx[q].at[0]))
    id_load = load(ids_hbm, ids_ref)
    small_loads = [load(ctx_hbm, ctx_ref), load(gate_hbm, gate_ref)]
    kv_loads = [
        load(ql_hbm, ql_ref),
        load(kl_hbm, kl_ref),
        load(qr_hbm, qr_ref),
        load(kr_hbm, kr_ref),
    ]

    lane_of = lax.broadcasted_iota(jnp.int32, (tok, lines), 1) & (tok - 1)
    spread = jnp.where(lax.broadcasted_iota(jnp.int32, (tok, lines), 0) == lane_of, 1.0, 0.0)
    spread = spread.astype(BF16)
    id_load.wait()
    my_ids = dot(ids_ref[...].astype(F32).astype(BF16), spread)
    ids0[...] = my_ids
    for made in hid_loads:
        made.wait()
    with jax.named_scope("barrier"):
        pl.semaphore_wait(barrier, 2 * (n - 1) + 1)

    id_copies = [copy(ids0, idr.at[off], s_id.at[:, off], on_a(off)) for off in order]
    for made in id_copies:
        made.start()
    g_copies = []
    for q, (at, w) in enumerate(cd):
        g_copies.append(
            [copy(gx[q].at[0], gx[q].at[off], s_g.at[:, q, off], on_a(off)) for off in order]
        )
        for made in g_copies[-1]:
            made.start()
    w_loads = [
        load(wg_hbm.at[pl.ds(own, half), :], wg.at[0]),
        load(wu_hbm.at[pl.ds(own, half), :], wu.at[0]),
        load(wg_hbm.at[pl.ds(oth, half), :], wg.at[1]),
        load(wu_hbm.at[pl.ds(oth, half), :], wu.at[1]),
        load(wd_hbm.at[:, pl.ds(own, half)], wdo),
    ]

    for made in small_loads + kv_loads:
        made.wait()
    nb, nh, lat = ql_ref.shape
    ctx = kl_ref.shape[1]
    per = nb * nh // n
    first = (y * n + x) * ctx
    for b in range(nb):
        scores = lax.dot_general(
            ql_ref[b], kl_ref[b], (((1,), (1,)), ((), ())), preferred_element_type=F32
        )
        scores = scores + dot(qr_ref[b], kr_ref[b])
        position = first + lax.broadcasted_iota(jnp.int32, scores.shape, 1)
        valid = position < ctx_ref[b]
        scores = jnp.where(valid, scores * softmax_scale, -1e30)
        peak = jnp.max(scores, axis=1, keepdims=True)
        probs = jnp.where(valid, jnp.exp(scores - peak), 0.0)
        total = jnp.sum(probs, axis=1, keepdims=True)
        weighted = dot(probs.astype(BF16), kl_ref[b])
        lane = lax.broadcasted_iota(jnp.int32, (nh, 128), 1)
        stats = jnp.where(lane < 64, peak, total)
        for k in range(nh // per):
            as0[b * (nh // per) + k, :, :lat] = weighted[k * per : (k + 1) * per]
            as0[b * (nh // per) + k, :, lat:] = stats[k * per : (k + 1) * per]
    a0 = []
    for off in order:
        block = lax.rem(A + off, n)
        a0.append(copy(as0.at[block], ar0.at[off], s_a.at[:, 0, off], on_a(off)))
        a0[-1].start()

    def joined(parts):
        peaks = [p[:, lat : lat + 1] for p in parts]
        totals = [p[:, lat + 64 : lat + 65] for p in parts]
        top = functools.reduce(jnp.maximum, peaks)
        scales = [jnp.exp(p - top) for p in peaks]
        total = sum(t * s for t, s in zip(totals, scales))
        weighted = sum(p[:, :lat] * s for p, s in zip(parts, scales))
        return top, total, weighted

    r_col = lax.broadcasted_iota(jnp.int32, (rows, 1), 0)

    def parts_of(r):
        q = lax.shift_right_logical(r * 171, 9)
        return lax.shift_right_logical(q, log), q & (n - 1), r - q * SLOTS

    first_of, second_of, slot_of = parts_of(r_col)
    arrive("ids", id_copies)
    lane_t = lax.broadcasted_iota(jnp.int32, (topk, lines), 1)
    line_ids = my_ids
    for off in range(1, n):
        line_ids = jnp.where(lane_t // tok == off, idr[off], line_ids)
    lane_1 = lax.broadcasted_iota(jnp.int32, (1, lines), 1)
    back = lane_1 // tok
    owner = sa * ((A - back + n) & (n - 1)) + sb * B
    live = owner * tok + (lane_1 & (tok - 1)) < batch_ref[0]
    wanted = (sa * A + sb * ((B + first_of) & (n - 1))).astype(F32)
    match = line_ids[0:1, :] == wanted
    for k in range(1, topk):
        match = match | (line_ids[k : k + 1, :] == wanted)
    match = match & live & (back == second_of)
    match = match.astype(F32)
    t_row = lax.broadcasted_iota(jnp.int32, (lines, lines), 0)
    t_col = lax.broadcasted_iota(jnp.int32, (lines, lines), 1)
    before = jnp.where(t_row < t_col, 1.0, 0.0).astype(BF16)
    rank = dot(match.astype(BF16), before)
    pick = jnp.where(rank == slot_of.astype(F32), match, 0.0).astype(BF16)

    swap_to = ((second_of << log) + first_of) * SLOTS + slot_of
    swap = jnp.where(lax.broadcasted_iota(jnp.int32, (rows, rows), 1) == swap_to, 1.0, 0.0).astype(
        BF16
    )

    x_copies = []
    for q, (at, w) in enumerate(cd):
        arrive(f"g{q}", g_copies[q])
        packed = dot(pick, gx[q][...].reshape(lines, w))
        xo[q][0] = packed[:blk].astype(BF16)
        for off in range(1, n):
            pk[q][off] = packed[off * blk : (off + 1) * blk].astype(BF16)
        x_copies.append(
            [copy(pk[q].at[off], xo[q].at[off], s_x.at[:, q, off], on_b(off)) for off in order]
        )
        for made in x_copies[-1]:
            made.start()

    w_copy = copy(wd_hbm.at[:, pl.ds(oth, half)], wdr, s_w, partner)
    w_copy.start()

    for made in w_loads:
        made.wait()
    for q, (at, w) in enumerate(cd):
        d_copies = [copy(xo[q].at[0], xx[q].at[0], s_d.at[:, q, 0], partner)]
        d_copies[0].start()
        for k, off in enumerate(reversed(order)):
            arrive(f"x{q}_{k}", [x_copies[q][len(order) - 1 - k]])
            d_copies.append(copy(xo[q].at[off], xx[q].at[off], s_d.at[:, q, off], partner))
            d_copies[-1].start()
        mine = xo[q][...].reshape(rows, w)
        gate = dot(mine, wg[0, at : at + w, :])
        upper = dot(mine, wu[0, at : at + w, :])
        if q:
            gate = gate + acc[:, :ff]
            upper = upper + acc[:, ff:]
        arrive(f"d{q}", d_copies)
        other = dot(swap, xx[q][...].reshape(rows, w)).astype(BF16)
        gate = gate + dot(other, wg[1, at : at + w, :])
        upper = upper + dot(other, wu[1, at : at + w, :])
        if q < len(cd) - 1:
            acc[:, :ff] = gate
            acc[:, ff:] = upper
    hidden = (gate / (1.0 + jnp.exp(-gate)) * upper).astype(BF16)
    hs[...] = hidden
    h_copy = copy(hs, hr, s_h, partner)
    h_copy.start()
    for q, (at, w) in enumerate(cr):
        va[q][...] = dot(hidden, wdo[:, at : at + w])
    arrive("a0", a0)
    top, total, weighted = joined([as0[A]] + [ar0[off] for off in range(1, n)])
    lane = lax.broadcasted_iota(jnp.int32, (per, 128), 1)
    as1[:, :lat] = weighted
    as1[:, lat:] = jnp.where(lane < 64, top, total)
    a1 = [copy(as1, ar1.at[off], s_a.at[:, 1, off], on_b(off)) for off in order]
    for made in a1:
        made.start()

    arrive("wcopy", [w_copy])
    arrive("h", [h_copy])
    turned = dot(swap, hr[...]).astype(BF16)

    v_copies = []
    for q, (at, w) in enumerate(cr):
        value = va[q][...] + dot(turned, wdr[:, at : at + w])
        vr[q][0] = value[:blk].astype(BF16)
        for off in range(1, n):
            vb[q][off] = value[off * blk : (off + 1) * blk].astype(BF16)
        v_copies.append(
            [copy(vb[q].at[off], vr[q].at[off], s_v.at[:, q, off], on_b(n - off)) for off in order]
        )
        for made in v_copies[-1]:
            made.start()

    named = (sa * ((A + first_of) & (n - 1)) + sb * ((B + second_of) & (n - 1))).astype(F32)
    gates = gate_ref[...]
    coarse = lax.shift_right_logical(gates, 5)
    fine = gates - coarse * 32
    coarse = dot(coarse.astype(F32).astype(BF16), spread)
    fine = dot(fine.astype(F32).astype(BF16), spread)
    my_gates = (coarse * 32.0 + fine) / gate_denominator
    here = jnp.zeros((rows, lines), F32)
    weight = jnp.zeros((rows, lines), F32)
    for k in range(topk):
        same = my_ids[k : k + 1, :] == named
        here = jnp.where(same, 1.0, here)
        weight = jnp.where(same, my_gates[k : k + 1, :], weight)
    token = (sa * A + sb * B) * tok + lane_1
    here = jnp.where((token < batch_ref[0]) & (lane_1 < tok), here, 0.0)
    rank = dot(here.astype(BF16), before)
    weight = jnp.where((rank == slot_of.astype(F32)) & (here > 0.0), weight, 0.0)
    weight = weight.T[:tok]
    high = weight.astype(BF16)
    low = (weight - high.astype(F32)).astype(BF16)

    u_copies = []
    for q, (at, w) in enumerate(cr):
        arrive(f"v{q}", v_copies[q])
        back_rows = dot(swap, vr[q][...].reshape(rows, w))
        ur[q][0] = back_rows[:blk].astype(BF16)
        for off in range(1, n):
            ub[q][off] = back_rows[off * blk : (off + 1) * blk].astype(BF16)
        u_copies.append(
            [copy(ub[q].at[off], ur[q].at[off], s_u.at[:, q, off], on_a(n - off)) for off in order]
        )
        for made in u_copies[-1]:
            made.start()
        if q:
            continue
        arrive("a1", a1)
        top, total, weighted = joined([as1[...]] + [ar1[off] for off in range(1, n)])
        as2[A] = (weighted / total).astype(BF16)
        a2 = [copy(as2.at[A], as2.at[A], s_a.at[:, 2, off], on_a(off)) for off in order]
        for made in a2:
            made.start()

    arrive("a2", a2)
    attn_ref[...] = as2[...].reshape(nb, nh, lat)

    o_copies = []
    for q, (at, w) in enumerate(cr):
        arrive(f"u{q}", u_copies[q])
        arrived = ur[q][...].reshape(rows, w)
        here_at = pl.ds(pl.multiple_of(own + at, 128), w)
        moe_ref[:, here_at] = (dot(high, arrived) + dot(low, arrived)).astype(BF16)
        o_copies.append(
            copy(moe_ref.at[:, here_at], moe_ref.at[:, here_at], s_o.at[:, q], partner)
        )
        o_copies[-1].start()
    arrive("o", o_copies)
    with jax.named_scope("sends"):
        for made in sent:
            made.wait_send()


def starts(widths):
    at, found = 0, []
    for w in widths:
        found.append((at, w))
        at += w
    return found


def local(
    hidden_in,
    batch_len,
    expert_ids,
    gate_num,
    w_gate,
    w_up,
    w_down,
    q_latent,
    q_rope,
    kv_latent,
    kv_rope,
    ctx_len,
):
    n = lax.axis_size("expert_0")
    tok, width = hidden_in.shape
    half = width // 2
    ff = w_gate.shape[2]
    nb, nh, lat = q_latent.shape
    per = nb * nh // n
    blk = n * SLOTS
    rows = n * blk
    cd = starts(split_widths(half, ND))
    cr = starts(split_widths(half, NR))
    topk = expert_ids.shape[1]
    lines = n * tok
    ctx = kv_latent.shape[1]
    hbm = pl.BlockSpec(memory_space=pltpu.HBM)
    vmem = pl.BlockSpec(memory_space=pltpu.VMEM)
    V = pltpu.VMEM
    dma = pltpu.SemaphoreType.DMA
    qd, qr = len(cd), len(cr)
    i32 = jnp.int32
    scratch = [
        pltpu.SMEM(ctx_len.shape, i32),
        V((topk, tok), i32),
        V((topk, tok), i32),
        V(q_latent.shape, BF16),
        V(q_rope.shape, BF16),
        V(kv_latent.shape, BF16),
        V(kv_rope.shape, BF16),
        V((2, half, ff), BF16),
        V((2, half, ff), BF16),
        V((ff, half), BF16),
        V((ff, half), BF16),
        V((topk, lines), F32),
        V((n, topk, lines), F32),
        [V((n, tok, w), BF16) for _, w in cd],
        [V((n, blk, w), BF16) for _, w in cd],
        [V((n, blk, w), BF16) for _, w in cd],
        [V((n, blk, w), BF16) for _, w in cd],
        V((rows, ff), BF16),
        V((rows, ff), BF16),
        [V((rows, w), F32) for _, w in cr],
        [V((n, blk, w), BF16) for _, w in cr],
        [V((n, blk, w), BF16) for _, w in cr],
        [V((n, blk, w), BF16) for _, w in cr],
        [V((n, blk, w), BF16) for _, w in cr],
        V((n, per, lat + 128), F32),
        V((n, per, lat + 128), F32),
        V((per, lat + 128), F32),
        V((n, per, lat + 128), F32),
        V((n, per, lat), BF16),
        V((rows, 2 * ff), F32),
        dma((qd + 12,)),
        dma((2,)),
        dma((2, n)),
        dma((2, qd, n)),
        dma((2, qd, n)),
        dma((2, qd, n)),
        dma((2,)),
        dma((2, qr, n)),
        dma((2, qr, n)),
        dma((2, 3, n)),
        dma((2, qr)),
    ]
    outs = (
        jax.ShapeDtypeStruct((tok, width), BF16),
        jax.ShapeDtypeStruct((nb, nh, lat), BF16),
    )
    return pl.pallas_call(
        functools.partial(kernel, n, cd, cr),
        out_shape=tuple(pltpu.VMEM(o.shape, o.dtype) for o in outs) if KEEP else outs,
        in_specs=[pl.BlockSpec(memory_space=pltpu.SMEM)] + [hbm] * 11,
        out_specs=(vmem, vmem),
        scratch_shapes=scratch,
        compiler_params=pltpu.CompilerParams(
            collective_id=0, has_side_effects=True, vmem_limit_bytes=52 * 1024 * 1024
        ),
        name="layer_step",
    )(
        batch_len,
        *(
            pltpu.with_memory_space_constraint(value, pltpu.HBM)
            for value in (
                ctx_len,
                expert_ids.T,
                gate_num.T,
                hidden_in,
                w_gate[0],
                w_up[0],
                w_down[0],
                q_latent,
                q_rope,
                kv_latent,
                kv_rope,
            )
        )
    )


def solution(mesh):
    owners = mesh.shape["expert"]
    side = 1
    while side * side < owners:
        side *= 2
    finer = Mesh(
        mesh.devices.reshape(mesh.shape["groups"], side, owners // side, mesh.shape["tensor"]),
        AXES,
    )
    in_specs = (
        P(GROUPS_EXPERT, None),
        P("groups"),
        P(GROUPS_EXPERT, None),
        P(GROUPS_EXPERT, None),
        P(EXPERT, None, "tensor"),
        P(EXPERT, None, "tensor"),
        P(EXPERT, "tensor", None),
        P("groups", "tensor", None),
        P("groups", "tensor", None),
        P("groups", EXPERT, None),
        P("groups", None, EXPERT),
        P("groups"),
    )
    out_specs = (P(GROUPS_EXPERT, None), P("groups", "tensor", None))
    return jax.shard_map(local, mesh=finer, in_specs=in_specs, out_specs=out_specs, check_vma=False)
```

```python
import functools

import jax
import jax.numpy as jnp
from jax import lax
from jax.experimental import pallas as pl
from jax.experimental.pallas import tpu as pltpu
from jax.sharding import Mesh
from jax.sharding import PartitionSpec as P

MESH = pl.DeviceIdType.MESH
EXPERT = ("expert_0", "expert_1")
GROUPS_EXPERT = ("groups", "expert_0", "expert_1")
AXES = ("groups", "expert_0", "expert_1", "tensor")

gate_denominator = 1024.0
softmax_scale = 192.0 ** (-0.5)
KEEP = True
GROUPS = ((0, 2), (2, 3))
ND = 2
NR = 1
THROTTLE = False
F32 = jnp.float32
BF16 = jnp.bfloat16


def split_widths(width, parts):
    unit = 256 if width % 256 == 0 else 128
    units = width // unit
    sizes = [units // parts + (1 if k < units % parts else 0) for k in range(parts)]
    return [s * unit for s in sizes if s]


def dot(a, b):
    return jnp.dot(a, b, preferred_element_type=F32)


def kernel(
    n,
    cd,
    cr,
    batch_ref,
    ctx_hbm,
    ids_hbm,
    gate_hbm,
    hid_hbm,
    wg_hbm,
    wu_hbm,
    wd_hbm,
    ql_hbm,
    qr_hbm,
    kl_hbm,
    kr_hbm,
    moe_ref,
    attn_ref,
    ctx_ref,
    ids_ref,
    gate_ref,
    ql_ref,
    qr_ref,
    kl_ref,
    kr_ref,
    wg,
    wu,
    wdo,
    wdr,
    ids0,
    idr,
    gx,
    pk,
    xo,
    xx,
    hs,
    hr,
    va,
    vb,
    vr,
    ub,
    ur,
    as0,
    ar0,
    as1,
    ar1,
    as2,
    acc,
    lsem,
    s_w,
    s_id,
    s_g,
    s_x,
    s_d,
    s_h,
    s_v,
    s_u,
    s_a,
    s_o,
):
    log = n.bit_length() - 1
    topk, tok = ids_ref.shape
    ff = wg.shape[2]
    half = hid_hbm.shape[1] // 2
    lines = n * tok
    g = lax.axis_index("groups")
    y = lax.axis_index("expert_0")
    x = lax.axis_index("expert_1")
    c = lax.axis_index("tensor")
    A = y + c * (x - y)
    B = x + c * (y - x)
    sa = n + c * (1 - n)
    sb = 1 + c * (n - 1)
    order = sorted(range(1, n), key=lambda k: (-min(k, n - k), k))
    own = pl.multiple_of(c * half, 128)
    oth = pl.multiple_of((1 - c) * half, 128)

    def on_a(off):
        p = lax.rem(A + off, n)
        return (g, p + c * (y - p), x + c * (p - x), c)

    def on_b(off):
        p = lax.rem(B + off, n)
        return (g, y + c * (p - y), p + c * (x - p), c)

    partner = (g, y, x, 1 - c)
    sent = []

    def copy(src, dst, sems, device):
        made = pltpu.make_async_remote_copy(
            src_ref=src,
            dst_ref=dst,
            send_sem=sems.at[0],
            recv_sem=sems.at[1],
            device_id=device,
            device_id_type=MESH,
        )
        sent.append(made)
        return made

    def arrive(name, copies):
        with jax.named_scope(name):
            for made in copies:
                made.wait_recv()

    barrier = pltpu.get_barrier_semaphore()
    for off in order:
        pl.semaphore_signal(barrier, inc=1, device_id=on_a(off), device_id_type=MESH)
        pl.semaphore_signal(barrier, inc=1, device_id=on_b(off), device_id_type=MESH)
    pl.semaphore_signal(barrier, inc=1, device_id=partner, device_id_type=MESH)

    started = []

    def load(src, dst):
        made = pltpu.make_async_copy(src, dst, lsem.at[len(started)])
        made.start()
        started.append(made)
        return made

    hid_loads = []
    for q, (at, w) in enumerate(cd):
        here_at = pl.ds(pl.multiple_of(own + at, 128), w)
        hid_loads.append(load(hid_hbm.at[:, here_at], gx[q].at[0]))
    id_load = load(ids_hbm, ids_ref)
    small_loads = [load(ctx_hbm, ctx_ref), load(gate_hbm, gate_ref)]
    kv_loads = [
        load(ql_hbm, ql_ref),
        load(kl_hbm, kl_ref),
        load(qr_hbm, qr_ref),
        load(kr_hbm, kr_ref),
    ]

    lane_of = lax.broadcasted_iota(jnp.int32, (tok, lines), 1) & (tok - 1)
    spread = jnp.where(lax.broadcasted_iota(jnp.int32, (tok, lines), 0) == lane_of, 1.0, 0.0)
    spread = spread.astype(BF16)
    id_load.wait()
    my_ids = dot(ids_ref[...].astype(F32).astype(BF16), spread)
    ids0[...] = my_ids
    for made in hid_loads:
        made.wait()
    with jax.named_scope("barrier"):
        pl.semaphore_wait(barrier, 2 * (n - 1) + 1)

    id_copies = [copy(ids0, idr.at[off], s_id.at[:, off], on_a(off)) for off in order]
    for made in id_copies:
        made.start()
    g_copies = []
    for q, (at, w) in enumerate(cd):
        g_copies.append(
            [copy(gx[q].at[0], gx[q].at[off], s_g.at[:, q, off], on_a(off)) for off in order]
        )
        for made in g_copies[-1]:
            made.start()
    w_loads = [
        load(wg_hbm.at[pl.ds(own, half), :], wg.at[0]),
        load(wu_hbm.at[pl.ds(own, half), :], wu.at[0]),
        load(wg_hbm.at[pl.ds(oth, half), :], wg.at[1]),
        load(wu_hbm.at[pl.ds(oth, half), :], wu.at[1]),
        load(wd_hbm.at[:, pl.ds(own, half)], wdo),
    ]
    w_copy = copy(wd_hbm.at[:, pl.ds(oth, half)], wdr, s_w, partner)
    w_copy.start()

    for made in small_loads + kv_loads:
        made.wait()
    nb, nh, lat = ql_ref.shape
    ctx = kl_ref.shape[1]
    per = nb * nh // n
    first = (y * n + x) * ctx
    for b in range(nb):
        scores = lax.dot_general(
            ql_ref[b], kl_ref[b], (((1,), (1,)), ((), ())), preferred_element_type=F32
        )
        scores = scores + dot(qr_ref[b], kr_ref[b])
        position = first + lax.broadcasted_iota(jnp.int32, scores.shape, 1)
        valid = position < ctx_ref[b]
        scores = jnp.where(valid, scores * softmax_scale, -1e30)
        peak = jnp.max(scores, axis=1, keepdims=True)
        probs = jnp.where(valid, jnp.exp(scores - peak), 0.0)
        total = jnp.sum(probs, axis=1, keepdims=True)
        weighted = dot(probs.astype(BF16), kl_ref[b])
        lane = lax.broadcasted_iota(jnp.int32, (nh, 128), 1)
        stats = jnp.where(lane < 64, peak, total)
        for k in range(nh // per):
            as0[b * (nh // per) + k, :, :lat] = weighted[k * per : (k + 1) * per]
            as0[b * (nh // per) + k, :, lat:] = stats[k * per : (k + 1) * per]
    a0 = []
    for off in order:
        block = lax.rem(A + off, n)
        a0.append(copy(as0.at[block], ar0.at[off], s_a.at[:, 0, off], on_a(off)))
        a0[-1].start()

    def joined(parts):
        peaks = [p[:, lat : lat + 1] for p in parts]
        totals = [p[:, lat + 64 : lat + 65] for p in parts]
        top = functools.reduce(jnp.maximum, peaks)
        scales = [jnp.exp(p - top) for p in peaks]
        total = sum(t * s for t, s in zip(totals, scales))
        weighted = sum(p[:, :lat] * s for p, s in zip(parts, scales))
        return top, total, weighted

    t_row = lax.broadcasted_iota(jnp.int32, (lines, lines), 0)
    t_col = lax.broadcasted_iota(jnp.int32, (lines, lines), 1)
    before = jnp.where(t_row < t_col, 1.0, 0.0).astype(BF16)
    lane_1 = lax.broadcasted_iota(jnp.int32, (1, lines), 1)
    back = lane_1 // tok
    owner = sa * ((A - back + n) & (n - 1)) + sb * B
    live = owner * tok + (lane_1 & (tok - 1)) < batch_ref[0]
    arrive("ids", id_copies)
    lane_t = lax.broadcasted_iota(jnp.int32, (topk, lines), 1)
    line_ids = my_ids
    for off in range(1, n):
        line_ids = jnp.where(lane_t // tok == off, idr[off], line_ids)

    picks, swaps, numbers = [], [], []
    for low_slot, high_slot in GROUPS:
        m = high_slot - low_slot
        rows = n * n * m
        r = lax.broadcasted_iota(jnp.int32, (rows, 1), 0)
        pair = lax.shift_right_logical(r, m.bit_length() - 1)
        first_of = lax.shift_right_logical(pair, log)
        second_of = pair & (n - 1)
        inner = r & (m - 1)
        slot_of = (low_slot + inner).astype(F32)
        numbers.append((first_of, second_of, slot_of))
        wanted = (sa * A + sb * ((B + first_of) & (n - 1))).astype(F32)
        match = line_ids[0:1, :] == wanted
        for k in range(1, topk):
            match = match | (line_ids[k : k + 1, :] == wanted)
        match = (match & live & (back == second_of)).astype(F32)
        rank = dot(match.astype(BF16), before)
        picks.append(jnp.where(rank == slot_of, match, 0.0).astype(BF16))
        swap_to = ((second_of << log) + first_of) * m + inner
        r_lane = lax.broadcasted_iota(jnp.int32, (rows, rows), 1)
        swaps.append(jnp.where(r_lane == swap_to, 1.0, 0.0).astype(BF16))

    def stored(value, blk, mine, others):
        mine[0] = value[:blk].astype(BF16)
        for off in range(1, n):
            others[off] = value[off * blk : (off + 1) * blk].astype(BF16)

    nq = len(cd)
    x_copies = [[None] * nq for _ in GROUPS]

    def send_picked(k, q):
        blk = n * (GROUPS[k][1] - GROUPS[k][0])
        stored(dot(picks[k], gx[q][...].reshape(lines, cd[q][1])), blk, xo[k][q], pk[k][q])
        x_copies[k][q] = [
            copy(pk[k][q].at[off], xo[k][q].at[off], s_x.at[:, k * nq + q, off], on_b(off))
            for off in order
        ]
        if k == 0 or not THROTTLE:
            for made in x_copies[k][q]:
                made.start()

    for q in range(nq):
        arrive(f"g{q}", g_copies[q])
        send_picked(0, q)
    for k in range(1, len(GROUPS)):
        for q in range(nq):
            send_picked(k, q)
    with jax.named_scope("wload"):
        for made in w_loads:
            made.wait()

    v_copies = []
    for k, (low_slot, high_slot) in enumerate(GROUPS):
        blk = n * (high_slot - low_slot)
        rows = n * blk
        for q, (at, w) in enumerate(cd):
            at_q = k * nq + q
            d_copies = [copy(xo[k][q].at[0], xx[k][q].at[0], s_d.at[:, at_q, 0], partner)]
            d_copies[0].start()
            for p, off in reversed(list(enumerate(order))):
                arrive(f"x{k}{q}_{off}", [x_copies[k][q][p]])
                d_copies.append(
                    copy(xo[k][q].at[off], xx[k][q].at[off], s_d.at[:, at_q, off], partner)
                )
                d_copies[-1].start()
            if THROTTLE and k == 0 and q == nq - 1:
                for later in x_copies[1:]:
                    for made in sum(later, []):
                        made.start()
            mine = xo[k][q][...].reshape(rows, w)
            gate = dot(mine, wg[0, at : at + w, :])
            upper = dot(mine, wu[0, at : at + w, :])
            if q:
                gate = gate + acc[:rows, :ff]
                upper = upper + acc[:rows, ff:]
            arrive(f"d{k}{q}", d_copies)
            other = dot(swaps[k], xx[k][q][...].reshape(rows, w)).astype(BF16)
            gate = gate + dot(other, wg[1, at : at + w, :])
            upper = upper + dot(other, wu[1, at : at + w, :])
            if q < nq - 1:
                acc[:rows, :ff] = gate
                acc[:rows, ff:] = upper
        hidden = (gate / (1.0 + jnp.exp(-gate)) * upper).astype(BF16)
        hs[k][...] = hidden
        h_copy = copy(hs[k], hr[k], s_h.at[:, k], partner)
        h_copy.start()
        for q, (at, w) in enumerate(cr):
            va[q][:rows] = dot(hidden, wdo[:, at : at + w])
        if k == 0:
            arrive("a0", a0)
            top, total, weighted = joined([as0[A]] + [ar0[off] for off in range(1, n)])
            lane = lax.broadcasted_iota(jnp.int32, (per, 128), 1)
            as1[:, :lat] = weighted
            as1[:, lat:] = jnp.where(lane < 64, top, total)
            a1 = [copy(as1, ar1.at[off], s_a.at[:, 1, off], on_b(off)) for off in order]
            for made in a1:
                made.start()
        if k == len(GROUPS) - 1:
            arrive("a1", a1)
            top, total, weighted = joined([as1[...]] + [ar1[off] for off in range(1, n)])
            as2[A] = (weighted / total).astype(BF16)
            a2 = [copy(as2.at[A], as2.at[A], s_a.at[:, 2, off], on_a(off)) for off in order]
            for made in a2:
                made.start()
        if k == 0:
            arrive("wcopy", [w_copy])
        arrive(f"h{k}", [h_copy])
        turned = dot(swaps[k], hr[k][...]).astype(BF16)
        v_copies.append([])
        for q, (at, w) in enumerate(cr):
            value = va[q][:rows] + dot(turned, wdr[:, at : at + w])
            stored(value, blk, vr[k][q], vb[k][q])
            made_now = [
                copy(
                    vb[k][q].at[off],
                    vr[k][q].at[off],
                    s_v.at[:, k * len(cr) + q, off],
                    on_b(n - off),
                )
                for off in order
            ]
            for made in made_now:
                made.start()
            v_copies[k].append(made_now)
    gates = gate_ref[...]
    coarse = lax.shift_right_logical(gates, 5)
    fine = gates - coarse * 32
    coarse = dot(coarse.astype(F32).astype(BF16), spread)
    fine = dot(fine.astype(F32).astype(BF16), spread)
    my_gates = (coarse * 32.0 + fine) / gate_denominator
    token = (sa * A + sb * B) * tok + lane_1
    mine_live = (token < batch_ref[0]) & (lane_1 < tok)
    weights = []
    for first_of, second_of, slot_of in numbers:
        named = sa * ((A + first_of) & (n - 1)) + sb * ((B + second_of) & (n - 1))
        named = named.astype(F32)
        here = jnp.zeros((named.shape[0], lines), F32)
        weight = jnp.zeros((named.shape[0], lines), F32)
        for k in range(topk):
            same = my_ids[k : k + 1, :] == named
            here = jnp.where(same, 1.0, here)
            weight = jnp.where(same, my_gates[k : k + 1, :], weight)
        here = jnp.where(mine_live, here, 0.0)
        rank = dot(here.astype(BF16), before)
        weight = jnp.where((rank == slot_of) & (here > 0.0), weight, 0.0)
        weight = weight.T[:tok]
        high = weight.astype(BF16)
        weights.append((high, (weight - high.astype(F32)).astype(BF16)))

    u_copies = []
    for k, (low_slot, high_slot) in enumerate(GROUPS):
        blk = n * (high_slot - low_slot)
        u_copies.append([])
        for q, (at, w) in enumerate(cr):
            arrive(f"v{k}{q}", v_copies[k][q])
            stored(dot(swaps[k], vr[k][q][...].reshape(n * blk, w)), blk, ur[k][q], ub[k][q])
            made_now = [
                copy(
                    ub[k][q].at[off],
                    ur[k][q].at[off],
                    s_u.at[:, k * len(cr) + q, off],
                    on_a(n - off),
                )
                for off in order
            ]
            for made in made_now:
                made.start()
            u_copies[k].append(made_now)
    o_copies = []
    for q, (at, w) in enumerate(cr):
        summed = jnp.zeros((tok, w), F32)
        for k, (high, low) in enumerate(weights):
            arrive(f"u{k}{q}", u_copies[k][q])
            arrived = ur[k][q][...].reshape(high.shape[1], w)
            summed = summed + dot(high, arrived) + dot(low, arrived)
        here_at = pl.ds(pl.multiple_of(own + at, 128), w)
        moe_ref[:, here_at] = summed.astype(BF16)
        o_copies.append(
            copy(moe_ref.at[:, here_at], moe_ref.at[:, here_at], s_o.at[:, q], partner)
        )
        o_copies[-1].start()
    arrive("a2", a2)
    attn_ref[...] = as2[...].reshape(nb, nh, lat)
    arrive("o", o_copies)
    with jax.named_scope("sends"):
        for made in sent:
            made.wait_send()


def starts(widths):
    at, found = 0, []
    for w in widths:
        found.append((at, w))
        at += w
    return found


def local(
    hidden_in,
    batch_len,
    expert_ids,
    gate_num,
    w_gate,
    w_up,
    w_down,
    q_latent,
    q_rope,
    kv_latent,
    kv_rope,
    ctx_len,
):
    n = lax.axis_size("expert_0")
    tok, width = hidden_in.shape
    half = width // 2
    ff = w_gate.shape[2]
    nb, nh, lat = q_latent.shape
    per = nb * nh // n
    blks = [n * (high - low) for low, high in GROUPS]
    most = n * max(blks)
    cd = starts(split_widths(half, ND))
    cr = starts(split_widths(half, NR))
    topk = expert_ids.shape[1]
    lines = n * tok
    ctx = kv_latent.shape[1]
    hbm = pl.BlockSpec(memory_space=pltpu.HBM)
    vmem = pl.BlockSpec(memory_space=pltpu.VMEM)
    V = pltpu.VMEM
    dma = pltpu.SemaphoreType.DMA
    qd, qr = len(cd), len(cr)
    i32 = jnp.int32
    kk = len(GROUPS)
    scratch = [
        pltpu.SMEM(ctx_len.shape, i32),
        V((topk, tok), i32),
        V((topk, tok), i32),
        V(q_latent.shape, BF16),
        V(q_rope.shape, BF16),
        V(kv_latent.shape, BF16),
        V(kv_rope.shape, BF16),
        V((2, half, ff), BF16),
        V((2, half, ff), BF16),
        V((ff, half), BF16),
        V((ff, half), BF16),
        V((topk, lines), F32),
        V((n, topk, lines), F32),
        [V((n, tok, w), BF16) for _, w in cd],
        [[V((n, blk, w), BF16) for _, w in cd] for blk in blks],
        [[V((n, blk, w), BF16) for _, w in cd] for blk in blks],
        [[V((n, blk, w), BF16) for _, w in cd] for blk in blks],
        [V((n * blk, ff), BF16) for blk in blks],
        [V((n * blk, ff), BF16) for blk in blks],
        [V((most, w), F32) for _, w in cr],
        [[V((n, blk, w), BF16) for _, w in cr] for blk in blks],
        [[V((n, blk, w), BF16) for _, w in cr] for blk in blks],
        [[V((n, blk, w), BF16) for _, w in cr] for blk in blks],
        [[V((n, blk, w), BF16) for _, w in cr] for blk in blks],
        V((n, per, lat + 128), F32),
        V((n, per, lat + 128), F32),
        V((per, lat + 128), F32),
        V((n, per, lat + 128), F32),
        V((n, per, lat), BF16),
        V((most, 2 * ff), F32),
        dma((qd + 12,)),
        dma((2,)),
        dma((2, n)),
        dma((2, qd, n)),
        dma((2, kk * qd, n)),
        dma((2, kk * qd, n)),
        dma((2, kk)),
        dma((2, kk * qr, n)),
        dma((2, kk * qr, n)),
        dma((2, 3, n)),
        dma((2, qr)),
    ]
    outs = (
        jax.ShapeDtypeStruct((tok, width), BF16),
        jax.ShapeDtypeStruct((nb, nh, lat), BF16),
    )
    return pl.pallas_call(
        functools.partial(kernel, n, cd, cr),
        out_shape=tuple(pltpu.VMEM(o.shape, o.dtype) for o in outs) if KEEP else outs,
        in_specs=[pl.BlockSpec(memory_space=pltpu.SMEM)] + [hbm] * 11,
        out_specs=(vmem, vmem),
        scratch_shapes=scratch,
        compiler_params=pltpu.CompilerParams(
            collective_id=0, has_side_effects=True, vmem_limit_bytes=52 * 1024 * 1024
        ),
        name="layer_step",
    )(
        batch_len,
        *(
            pltpu.with_memory_space_constraint(value, pltpu.HBM)
            for value in (
                ctx_len,
                expert_ids.T,
                gate_num.T,
                hidden_in,
                w_gate[0],
                w_up[0],
                w_down[0],
                q_latent,
                q_rope,
                kv_latent,
                kv_rope,
            )
        )
    )


def solution(mesh):
    owners = mesh.shape["expert"]
    side = 1
    while side * side < owners:
        side *= 2
    finer = Mesh(
        mesh.devices.reshape(mesh.shape["groups"], side, owners // side, mesh.shape["tensor"]),
        AXES,
    )
    in_specs = (
        P(GROUPS_EXPERT, None),
        P("groups"),
        P(GROUPS_EXPERT, None),
        P(GROUPS_EXPERT, None),
        P(EXPERT, None, "tensor"),
        P(EXPERT, None, "tensor"),
        P(EXPERT, "tensor", None),
        P("groups", "tensor", None),
        P("groups", "tensor", None),
        P("groups", EXPERT, None),
        P("groups", None, EXPERT),
        P("groups"),
    )
    out_specs = (P(GROUPS_EXPERT, None), P("groups", "tensor", None))
    return jax.shard_map(local, mesh=finer, in_specs=in_specs, out_specs=out_specs, check_vma=False)
```
